32 devices in a mesh: grp: 4 (over y, x), tile: 8 (over z, core).
Axes of the slice: x: 2, y: 2, z: 4, core: 2. Of those that a mesh axis runs over, the one named last changes fastest.
Arguments:
- latents: bfloat16 [4, 1024, 1152], P('grp', 'tile'), may hold values from -6 to 6
- condition: bfloat16 [4, 1152], replicated, may hold values from -6 to 6
- w_modulate: bfloat16 [1152, 3456], P(None, 'grp'), may hold values from -1 to 1
- w_project: bfloat16 [1152, 3456], replicated, may hold values from -0.1875 to 0.1875
- w_output: bfloat16 [1152, 1152], replicated, may hold values from -0.1875 to 0.1875
- detail: int32 [4, 8], P('grp'), may hold values from 0 to 1, as said below
Outputs:
- updated: bfloat16 [4, 1024, 1152], P('grp', 'tile')
The draws below stay inside these ranges and needn't reach their ends.
Inputs may be any that keep to these rules, and one draw needn't show every extreme that they name: `detail`: at most 2 strips of an image are marked, and at least one.
All inputs are finite; a program needn't handle non-finite values.
Results may differ from the reference program's by a relative error of at most 0.012.
Values may be sent and summed in bfloat16 or wider, within the bound.
No kernel may reach another device: no remote copies, remote signals or barrier semaphores. Data moves between devices by JAX's collectives and lax.ppermute only.
A program may use at most 192 MiB of HBM per device.

```python
import math
import jax
import jax.numpy as jnp
from jax import lax

D = 1152
HEADS = 16
HEAD = 72
ROW_TOKENS = 64
TOK_DEV = 128
TILES = 8
MARKED = 2
TOKENS = 1024
IMAGES = 4


def draw_w_modulate(key, part):
    base = jax.random.normal(key, (D, 3 * D), jnp.float32)
    values = jnp.clip(base, -6.0, 6.0) / math.sqrt(4.0 * D)
    return values.astype(jnp.bfloat16)


def draw_detail(key, part):
    count_key = jax.random.fold_in(key, 11)
    image_key = jax.random.fold_in(key, 23)
    order_key = jax.random.fold_in(key, 37)
    counts = jax.random.randint(count_key, (IMAGES,), 1, MARKED + 1)
    chosen = jax.random.randint(image_key, (), 0, IMAGES)
    counts = jnp.where(jnp.arange(IMAGES, dtype=jnp.int32) == chosen, MARKED, counts)
    image_keys = jax.random.split(order_key, IMAGES)

    def one_order(subkey):
        return jax.random.permutation(subkey, TILES)
    orders = jax.vmap(one_order)(image_keys)
    return (orders < counts[:, None]).astype(jnp.int32)


def level_of(stream_key, dims, cuts, low, top_value):
    gain, own = 1.0, jax.random.fold_in(stream_key, 6)
    for position, blocks in cuts:
        draws = jnp.exp(jax.random.uniform(jax.random.fold_in(own, position), (blocks,), jnp.float32, low / len(cuts), top_value / len(cuts)))
        gain = gain * jnp.repeat(draws, dims[position] // blocks).reshape([-1 if axis == position else 1 for axis in range(len(dims))])
    return gain


def bell_draw(own_key, shape, width, bound, pieces=(), held_as=jnp.bfloat16):
    values = width * jax.random.normal(own_key, shape, jnp.float32)
    if pieces:
        values = values * level_of(own_key, shape, pieces, -0.22, 0.18)
    return jnp.clip(values, -bound, bound).astype(held_as)


def setup_inputs(seed: int = 0) -> dict:
    key_of = jax.random.split(jax.random.key(seed), 7)
    latents = bell_draw(key_of[0], (IMAGES, TOKENS, D), 1.0, 6.0, ((0, 4), (1, 8)))
    condition = bell_draw(key_of[1], (IMAGES, D), 1.0, 6.0)
    w_modulate = draw_w_modulate(jax.random.fold_in(key_of[6], 71), 0)
    w_project = bell_draw(key_of[3], (D, 3 * D), D ** -0.5, 0.1875)
    w_output = bell_draw(key_of[4], (D, D), D ** -0.5, 0.1875)
    detail = draw_detail(jax.random.fold_in(key_of[6], 71), 0)
    return {"latents": latents, "condition": condition, "w_modulate": w_modulate, "w_project": w_project, "w_output": w_output, "detail": detail}


def attend(query, keys, values, valid):
    count = query.shape[0]
    heads_q = query.astype(jnp.float32).reshape(count, HEADS, HEAD)
    heads_k = keys.astype(jnp.float32).reshape(keys.shape[0], HEADS, HEAD)
    heads_v = values.astype(jnp.float32).reshape(values.shape[0], HEADS, HEAD)
    scores = jnp.einsum('qhd,khd->hqk', heads_q, heads_k) / jnp.sqrt(jnp.float32(HEAD))
    scores = jnp.where(valid[None, None, :], scores, jnp.float32(-1e+30))
    top = lax.optimization_barrier(jnp.max(scores, axis=2, keepdims=True))
    probs = jnp.exp(scores - top)
    total = lax.optimization_barrier(jnp.sum(probs, axis=2))
    weights = probs.astype(jnp.bfloat16).astype(jnp.float32)
    result = jnp.einsum('hqk,khd->qhd', weights, heads_v)
    return (result / jnp.transpose(total)[:, :, None]).reshape(count, D)

def reference(latents, condition, w_modulate, w_project, w_output, detail):
    modulation = jnp.dot(condition, w_modulate, preferred_element_type=jnp.float32)
    shift = modulation[:, :D]
    scale = modulation[:, D:2 * D]
    gate = modulation[:, 2 * D:]

    def one_image(packed):
        tokens, shift_row, scale_row, gate_row, marks = packed
        values32 = tokens.astype(jnp.float32)
        mean = lax.optimization_barrier(jnp.mean(values32, axis=1, keepdims=True))
        centered = values32 - mean
        variance = lax.optimization_barrier(jnp.mean(centered * centered, axis=1, keepdims=True))
        normed = (centered / jnp.sqrt(variance + 1e-06) * (1.0 + scale_row) + shift_row).astype(jnp.bfloat16)
        projected = jnp.dot(normed, w_project, preferred_element_type=jnp.float32).astype(jnp.bfloat16)
        query = projected[:, :D].reshape(TILES, TOK_DEV, D)
        pairs = projected[:, D:]
        strips = pairs.reshape(TILES, TOK_DEV, 2 * D)
        blank = jnp.zeros((1, ROW_TOKENS, 2 * D), jnp.bfloat16)
        before = jnp.concatenate([blank, strips[:-1, TOK_DEV - ROW_TOKENS:]], axis=0)
        after = jnp.concatenate([strips[1:, :ROW_TOKENS], blank], axis=0)
        extended = jnp.concatenate([before, strips, after], axis=1)
        tile_ids = jnp.arange(TILES, dtype=jnp.int32)
        lower = jnp.broadcast_to((tile_ids > 0)[:, None], (TILES, ROW_TOKENS))
        upper = jnp.broadcast_to((tile_ids < TILES - 1)[:, None], (TILES, ROW_TOKENS))
        inner = jnp.ones((TILES, TOK_DEV), dtype=bool)
        valid = jnp.concatenate([lower, inner, upper], axis=1)
        all_valid = jnp.ones((TOKENS,), dtype=bool)

        def strip_work(item):
            strip_q, strip_kv, strip_valid, mark = item
            near = attend(strip_q, strip_kv[:, :D], strip_kv[:, D:], strip_valid)
            whole = attend(strip_q, pairs[:, :D], pairs[:, D:], all_valid)
            return (near + mark.astype(jnp.float32) * whole).astype(jnp.bfloat16)
        mixed = lax.map(strip_work, (query, extended, valid, marks)).reshape(TOKENS, D)
        branch = jnp.dot(mixed, w_output, preferred_element_type=jnp.float32)
        return (values32 + gate_row * branch).astype(jnp.bfloat16)
    return lax.map(one_image, (latents, shift, scale, gate, detail))
```

```python
import functools
import jax
import jax.numpy as jnp
from jax import lax
from jax.experimental import pallas as pl
from jax.experimental.pallas import tpu as pltpu
from jax.sharding import PartitionSpec as P

HEADS = 16
ROW_TOKENS = 64
LANES = 128
EPS = 1e-06
LOG2E = 1.4426950408889634
F32 = jnp.float32
BF16 = jnp.bfloat16


def window_of(head, size):
    first = head * size // LANES * LANES
    last = -(-((head + 1) * size) // LANES) * LANES
    return first, last


def head_mask(head, size, first, last):
    column = lax.broadcasted_iota(jnp.int32, (1, last - first), 1) + first
    return (column >= head * size) & (column < (head + 1) * size)


def assemble_modulation(pieces, row, blocks):
    here = lax.axis_index("grp")
    count = len(pieces)
    for back, piece in enumerate(pieces):
        blocks[lax.rem(here - back + count, count)] = piece[...]
    wide = pieces[0].shape[1]
    for block in range(count):
        row[:, block * wide : (block + 1) * wide] = blocks[block]


def normalize(rows, shift, scale):
    values = rows.astype(F32)
    mean = jnp.mean(values, axis=1, keepdims=True)
    centered = values - mean
    variance = jnp.mean(centered * centered, axis=1, keepdims=True)
    return (centered * lax.rsqrt(variance + EPS) * scale + shift).astype(BF16)


def attend_head(query, keys, values, head, size, bias):
    first, last = window_of(head, size)
    mask = head_mask(head, size, first, last)
    masked = jnp.where(mask, query[:, first:last].astype(F32), 0.0).astype(BF16)
    scores = lax.dot_general(
        masked, keys[:, first:last], (((1,), (1,)), ((), ())), preferred_element_type=F32
    )
    if bias is not None:
        scores = scores + bias
    top = jnp.max(scores, axis=1, keepdims=True)
    probs = jnp.exp2((scores - top) * (LOG2E / size**0.5))
    total = jnp.sum(probs, axis=1, keepdims=True)
    result = jnp.dot(probs.astype(BF16), values[:, first:last], preferred_element_type=F32)
    return first, last, mask, result * (1.0 / total)


def near_kernel(
    own, partner, across, *rest, parts
):
    pieces = rest[:parts]
    w_hbm, q_out, near_out, blocks, row, normed, w, kv, sems = rest[parts:]
    width = own.shape[1]
    count = own.shape[0]
    chunk = w.shape[2]
    chunks = w.shape[0]
    copies = [
        pltpu.make_async_copy(w_hbm.at[:, i * chunk : (i + 1) * chunk], w.at[i], sems.at[i])
        for i in range(chunks)
    ]
    for copy in copies:
        copy.start()
    place = lax.axis_index("tile")
    strips = lax.axis_size("tile")
    core = lax.rem(place, 2)
    assemble_modulation(pieces, row, blocks)
    shift = row[:, :width]
    scale = 1.0 + row[:, width : 2 * width]
    edge = ROW_TOKENS
    first = core == 0
    before = jnp.where(first, across[count - edge :], partner[count - edge :])
    after = jnp.where(first, partner[:edge], across[:edge])
    normed[:count] = normalize(own[...], shift, scale)
    normed[count : count + edge] = normalize(before, shift, scale)
    normed[count + edge :] = normalize(after, shift, scale)
    per = chunks // 3
    for i in range(chunks):
        copies[i].wait()
        if i < per:
            q_out[:, i * chunk : (i + 1) * chunk] = jnp.dot(
                normed[:count], w[i], preferred_element_type=F32
            ).astype(BF16)
        else:
            j = i - per
            kv[:, j * chunk : (j + 1) * chunk] = jnp.dot(
                normed[...], w[i], preferred_element_type=F32
            ).astype(BF16)
    column = lax.broadcasted_iota(jnp.int32, (1, count + 2 * edge), 1)
    hidden = ((place == 0) & (column >= count) & (column < count + edge)) | (
        (place == strips - 1) & (column >= count + edge)
    )
    bias = jnp.where(hidden, -1e30, 0.0)
    size = width // HEADS
    near_out[...] = jnp.zeros_like(near_out)
    for head in range(HEADS):
        lo, hi, mask, result = attend_head(q_out, kv, kv.at[:, width:], head, size, bias)
        near_out[:, lo:hi] = jnp.where(mask, result, near_out[:, lo:hi])


def whole_kernel(*refs, parts, pairs):
    own, partner = refs[:2]
    mine = refs[2 : 2 + pairs * 2]
    theirs = refs[2 + pairs * 2 : 2 + pairs * 4]
    refs = refs[2 + pairs * 4 :]
    pieces = refs[:parts]
    (
        marks, query, near, w_hbm, wo_hbm, out,
        blocks, row, raw, wkv, wo, kv, mixed, sem_o, sem_w, sem_x,
    ) = refs[parts:]
    width = own.shape[1]
    count = own.shape[0]
    place = lax.axis_index("tile")
    strips = lax.axis_size("tile")
    core = lax.rem(place, 2)
    chip = place // 2
    marked = marks[0, place] > 0
    copy_o = pltpu.make_async_copy(wo_hbm, wo, sem_o)
    copy_o.start()
    assemble_modulation(pieces, row, blocks)
    mixed[...] = near[...]
    size = width // HEADS

    @pl.when(marked)
    def _():
        copy_w = pltpu.make_async_copy(w_hbm.at[:, width:], wkv, sem_w)
        copy_w.start()
        pltpu.make_async_copy(own, raw.at[pl.ds(0, count)], sem_x).start()
        pltpu.make_async_copy(partner, raw.at[pl.ds(count, count)], sem_x).start()
        lefts = chip
        rights = strips // 2 - 1 - chip
        for side, (strips_of, ours) in enumerate(((mine, True), (theirs, False))):
            is_left = (core == 0) if ours else (core == 1)
            have = jnp.where(is_left, lefts, rights)
            base = jnp.where(is_left, 0, lefts)
            for d in range(pairs):

                @pl.when(d < have)
                def _(d=d, base=base, strips_of=strips_of):
                    for k in range(2):
                        at = pl.multiple_of((2 + 2 * (base + d) + k) * count, count)
                        pltpu.make_async_copy(
                            strips_of[2 * d + k], raw.at[pl.ds(at, count)], sem_x
                        ).start()

        pltpu.make_async_copy(raw, raw, sem_x).wait()
        shift = row[:, :width]
        scale = 1.0 + row[:, width : 2 * width]
        block = 64

        @pl.loop(0, raw.shape[0] // block)
        def _(i):
            at = pl.multiple_of(i * block, block)
            raw[pl.ds(at, block)] = normalize(raw[pl.ds(at, block)], shift, scale)

        copy_w.wait()
        chunk = 256

        @pl.loop(0, 2 * width // chunk)
        def _(i):
            at = pl.multiple_of(i * chunk, chunk)
            kv[:, pl.ds(at, chunk)] = jnp.dot(
                raw[...], wkv[:, pl.ds(at, chunk)], preferred_element_type=F32
            ).astype(BF16)

        for head in range(HEADS):
            lo, hi, mask, result = attend_head(query, kv, kv.at[:, width:], head, size, None)
            mixed[:, lo:hi] = mixed[:, lo:hi] + jnp.where(mask, result, 0.0)

    copy_o.wait()
    branch = jnp.dot(mixed[...].astype(BF16), wo[...], preferred_element_type=F32)
    gate = row[:, 2 * width : 3 * width]
    out[...] = (own[...].astype(F32) + gate * branch).astype(BF16)


def gather_strips(own):
    count = lax.axis_size("tile")
    chips = count // 2
    swap = [(i, i ^ 1) for i in range(count)]
    partner = lax.ppermute(own, "tile", swap)
    cross = [(2 * z + 1, 2 * z + 2) for z in range(chips - 1)]
    cross = cross + [(b, a) for a, b in cross]
    along = [(2 * z, 2 * z + 2) for z in range(chips - 1)]
    along = along + [(2 * z + 3, 2 * z + 1) for z in range(chips - 1)]
    first = lax.ppermute(own, "tile", cross)
    second = lax.ppermute(own, "tile", along)
    mine = [first, second]
    for _ in range(chips - 2):
        first = lax.ppermute(first, "tile", along)
        second = lax.ppermute(second, "tile", along)
        mine += [first, second]
    theirs = [lax.ppermute(strip, "tile", swap) for strip in mine]
    return partner, mine, theirs


def exchange_modulation(columns):
    count = lax.axis_size("grp")
    here = lax.axis_index("grp")
    pieces = [lax.dynamic_slice_in_dim(columns, here, 1, 0)]
    for ahead in range(1, count):
        row = lax.dynamic_slice_in_dim(columns, lax.rem(here + ahead, count), 1, 0)
        pieces.append(lax.ppermute(row, "grp", [(i, (i + ahead) % count) for i in range(count)]))
    return pieces


def on_device(latents, condition, w_modulate, w_project, w_output, detail):
    width = w_output.shape[0]
    own = latents[0]
    count = own.shape[0]
    columns = jnp.dot(condition, w_modulate, preferred_element_type=F32)
    pieces = exchange_modulation(columns)
    partner, mine, theirs = gather_strips(own)
    parts = len(pieces)
    wide = pieces[0].shape[1]
    rows = count + 2 * ROW_TOKENS
    vmem = pl.BlockSpec(memory_space=pltpu.VMEM)
    anywhere = pl.BlockSpec(memory_space=pl.ANY)
    chunks, chunk = 9, width // 3
    modulation_scratch = [
        pltpu.VMEM((parts, 1, wide), F32),
        pltpu.VMEM((1, 3 * width), F32),
    ]
    query, near = pl.pallas_call(
        functools.partial(near_kernel, parts=parts),
        name="near",
        out_shape=[
            jax.ShapeDtypeStruct((count, width), BF16),
            jax.ShapeDtypeStruct((count, width), F32),
        ],
        in_specs=[vmem] * (3 + parts) + [anywhere],
        out_specs=[vmem, vmem],
        scratch_shapes=modulation_scratch
        + [
            pltpu.VMEM((rows, width), BF16),
            pltpu.VMEM((chunks, width, chunk), BF16),
            pltpu.VMEM((rows, 2 * width), BF16),
            pltpu.SemaphoreType.DMA((chunks,)),
        ],
        cost_estimate=pl.CostEstimate(
            flops=2 * rows * width * 3 * width, bytes_accessed=6 * width * width, transcendentals=0
        ),
        compiler_params=pltpu.CompilerParams(vmem_limit_bytes=40 * 1024 * 1024),
    )(own, partner, mine[0], *pieces, w_project)
    tokens = count * lax.axis_size("tile")
    updated = pl.pallas_call(
        functools.partial(whole_kernel, parts=parts, pairs=len(mine) // 2),
        name="whole",
        out_shape=jax.ShapeDtypeStruct((count, width), BF16),
        in_specs=[vmem]
        + [anywhere] * (1 + 2 * len(mine))
        + [vmem] * parts
        + [pl.BlockSpec(memory_space=pltpu.SMEM), vmem, vmem, anywhere, anywhere],
        out_specs=vmem,
        scratch_shapes=modulation_scratch
        + [
            pltpu.VMEM((tokens, width), BF16),
            pltpu.VMEM((width, 2 * width), BF16),
            pltpu.VMEM((width, width), BF16),
            pltpu.VMEM((tokens, 2 * width), BF16),
            pltpu.VMEM((count, width), F32),
            pltpu.SemaphoreType.DMA,
            pltpu.SemaphoreType.DMA,
            pltpu.SemaphoreType.DMA,
        ],
        cost_estimate=pl.CostEstimate(
            flops=2 * tokens * width * 2 * width, bytes_accessed=6 * width * width, transcendentals=0
        ),
        compiler_params=pltpu.CompilerParams(vmem_limit_bytes=60 * 1024 * 1024),
    )(own, partner, *mine, *theirs, *pieces, detail, query, near, w_project, w_output)
    return updated[None]


def solution(mesh):
    in_specs = (P("grp", "tile", None), P(), P(None, "grp"), P(), P(), P("grp", None))
    out_specs = P("grp", "tile", None)
    return jax.shard_map(
        on_device, mesh=mesh, in_specs=in_specs, out_specs=out_specs, check_vma=False
    )
```

```python
import functools
import jax
import jax.numpy as jnp
from jax import lax
from jax.experimental import pallas as pl
from jax.experimental.pallas import tpu as pltpu
from jax.sharding import PartitionSpec as P

HEADS = 16
ROW_TOKENS = 64
LANES = 128
EPS = 1e-06
LOG2E = 1.4426950408889634
F32 = jnp.float32
BF16 = jnp.bfloat16


def half_columns(width):
    first = width // 2 // LANES * LANES
    return first, width - first


def assemble_modulation(pieces, row, blocks):
    here = lax.axis_index("grp")
    count = len(pieces)
    for back, piece in enumerate(pieces):
        blocks[lax.rem(here - back + count, count)] = piece[...]
    wide = pieces[0].shape[1]
    for block in range(count):
        row[:, block * wide : (block + 1) * wide] = blocks[block]


def normalize(rows, shift, scale):
    values = rows.astype(F32)
    mean = jnp.mean(values, axis=1, keepdims=True)
    centered = values - mean
    variance = jnp.mean(centered * centered, axis=1, keepdims=True)
    return (centered * lax.rsqrt(variance + EPS) * scale + shift).astype(BF16)


def normalize_rows(source, start, target, at, rows, shift, scale, block=32):
    for i in range(0, rows, block):
        target[pl.ds(at + i, block)] = normalize(source[pl.ds(start + i, block)], shift, scale)


def head_window(head, size, width, core):
    first, wide = half_columns(width)
    extra = width // 2 - first
    lo = head * size // LANES * LANES
    hi = min(-(-((head + 1) * size + extra) // LANES) * LANES, wide)
    column = lax.broadcasted_iota(jnp.int32, (1, hi - lo), 1) + (lo - head * size) - core * extra
    return lo, hi, (column >= 0) & (column < size)


def attend_heads(heads, size, width, core, query, keys, values, bias, scores, probs, target):
    windows = [head_window(head, size, width, core) for head in heads]
    bounds = [0]
    for key in keys:
        bounds.append(bounds[-1] + key.shape[0])
    spans = [slice(a, b) for a, b in zip(bounds, bounds[1:])]
    for head, (lo, hi, mask) in zip(heads, windows):
        part = query[:, lo:hi]
        masked = jnp.where(mask, part, jnp.zeros_like(part))
        for span, key in zip(spans, keys):
            scores[head - heads[0], :, span] = lax.dot_general(
                masked, key[:, lo:hi], (((1,), (1,)), ((), ())), preferred_element_type=F32
            )
    inverse = []
    for head in heads:
        score = scores[head - heads[0]]
        if bias is not None:
            score = score + bias
        top = jnp.max(score, axis=1, keepdims=True)
        prob = jnp.exp2((score - top) * (LOG2E / size**0.5))
        inverse.append(1.0 / jnp.sum(prob, axis=1, keepdims=True))
        probs[head - heads[0]] = prob.astype(BF16)
    for at, (head, (lo, hi, mask)) in enumerate(zip(heads, windows)):
        result = sum(
            jnp.dot(probs[at, :, span], value[:, lo:hi], preferred_element_type=F32)
            for span, value in zip(spans, values)
        )
        target[:, lo:hi] += jnp.where(mask, result * inverse[at], 0.0)


def modulate_kernel(condition, w, *outs):
    columns = jnp.dot(condition[...], w[...], preferred_element_type=F32)
    here = lax.axis_index("grp")
    count = len(outs)
    which = lax.broadcasted_iota(jnp.int32, (columns.shape[0], 1), 0)
    for ahead, out in enumerate(outs):
        out[...] = jnp.sum(
            jnp.where(which == lax.rem(here + ahead, count), columns, 0.0), axis=0, keepdims=True
        )


def project_kernel(own, partner, mine, theirs, *rest, parts):
    pieces = rest[:parts]
    w, query, kv, blocks, row, normed = rest[parts:]
    count, width = own.shape
    first, wide = half_columns(width)
    core = lax.rem(lax.axis_index("tile"), 2)
    assemble_modulation(pieces, row, blocks)
    shift = row[:, :width]
    scale = 1.0 + row[:, width : 2 * width]
    edge = ROW_TOKENS
    end = edge + 2 * count
    other = 1 - core
    normalize_rows(own, 0, normed, pl.multiple_of(edge + count * core, edge), count, shift, scale)
    normalize_rows(partner, 0, normed, pl.multiple_of(edge + count * other, edge), count, shift, scale)
    inner = count - edge
    normalize_rows(
        mine, pl.multiple_of(inner * other, edge), normed, pl.multiple_of(end * core, edge), edge, shift, scale
    )
    normalize_rows(
        theirs, pl.multiple_of(inner * core, edge), normed, pl.multiple_of(end * other, edge), edge, shift, scale
    )
    at = [pl.multiple_of(section * width + first * core, LANES) for section in range(3)]
    query[...] = jnp.dot(normed[edge:end], w[:, pl.ds(at[0], wide)], preferred_element_type=F32).astype(BF16)
    for section in (1, 2):
        part = slice((section - 1) * wide, section * wide)
        kv[:, part] = jnp.dot(normed[...], w[:, pl.ds(at[section], wide)], preferred_element_type=F32).astype(BF16)


def attend_kernel(query, kv, near, scores, probs, *, size):
    edge = ROW_TOKENS
    count = query.shape[0] // 2
    wide = query.shape[1]
    core, chip, chips = place_of_chip()
    column = lax.broadcasted_iota(jnp.int32, (1, count + 2 * edge), 1)
    near[...] = jnp.zeros_like(near)
    for strip in range(2):
        rows = pl.ds(strip * count, count)
        keys = pl.ds(strip * count, count + 2 * edge)
        if strip == 0:
            hidden = (chip == 0) & (column < edge)
        else:
            hidden = (chip == chips - 1) & (column >= count + edge)
        bias = jnp.where(hidden, -1e30, 0.0)
        attend_heads(
            range(HEADS // 2), size, size * HEADS, core, query.at[rows],
            [kv.at[keys, :wide]], [kv.at[keys, wide:]], bias, scores.at[strip], probs.at[strip], near.at[rows],
        )


def place_of_chip():
    place = lax.axis_index("tile")
    return lax.rem(place, 2), place // 2, lax.axis_size("tile") // 2


def chip_marks(marks, chip):
    return [marks[0, 2 * chip] > 0, marks[0, 2 * chip + 1] > 0]


def project_pairs(raw, pairs, row, w, kv, start, width, core):
    shift = row[:, :width]
    scale = 1.0 + row[:, width : 2 * width]
    first, wide = half_columns(width)
    block = 2 * LANES

    @pl.loop(0, pairs)
    def _(i):
        at = pl.multiple_of(i * block, block)
        normalize_rows(raw, at, raw, at, block, shift, scale)
        for section in range(2):
            columns = pl.ds(pl.multiple_of((section + 1) * width + first * core, LANES), wide)
            kv[pl.ds(start + at, block), section * wide : (section + 1) * wide] = jnp.dot(
                raw[pl.ds(at, block)], w[:, columns], preferred_element_type=F32
            ).astype(BF16)


def early_kernel(*refs, parts, depth):
    mine = refs[: 2 * depth]
    theirs = refs[2 * depth : 4 * depth]
    refs = refs[4 * depth :]
    pieces = refs[:parts]
    marks, around, w, kv, blocks, row, raw, sem = refs[parts:]
    count, width = mine[0].shape
    core, chip, chips = place_of_chip()
    marked = chip_marks(marks, chip)
    inner = 2 * count

    @pl.when(marked[0] | marked[1])
    def _():
        def each_strip(act):
            for ours in (True, False):
                strips_of = mine if ours else theirs
                is_left = (core == 0) if ours else (core == 1)
                have = jnp.where(is_left, chip, chips - 1 - chip)
                base = jnp.where(is_left, 0, jnp.minimum(chip, depth))
                for d in range(depth):

                    @pl.when(d < have)
                    def _(d=d, base=base, strips_of=strips_of):
                        for k in range(2):
                            at = pl.multiple_of((2 * (base + d) + k) * count, count)
                            act(pltpu.make_async_copy(strips_of[2 * d + k], raw.at[pl.ds(at, count)], sem))

        each_strip(lambda copy: copy.start())
        kv[:inner] = around[ROW_TOKENS : ROW_TOKENS + inner]
        assemble_modulation(pieces, row, blocks)
        each_strip(lambda copy: copy.wait())
        pairs = jnp.minimum(chip, depth) + jnp.minimum(chips - 1 - chip, depth)
        project_pairs(raw, pairs, row, w, kv, inner, width, core)


def late_kernel(mine0, mine1, theirs0, theirs1, *refs, parts):
    pieces = refs[:parts]
    marks, query, most, near, w, keep, send, blocks, row, raw, last, whole, scores, probs, sem = refs[parts:]
    count, width = mine0.shape
    _, wide = half_columns(width)
    core, chip, chips = place_of_chip()
    marked = chip_marks(marks, chip)
    size = width // HEADS
    bulk = most.shape[0] - 2 * count
    whole[...] = jnp.zeros_like(whole)

    @pl.when(marked[0] | marked[1])
    def _():
        at_end = (chip == 0) | (chip == chips - 1)
        from_mine = (chip == 0) == (core == 1)

        @pl.when(at_end)
        def _():
            def start(pair):
                for k, strip in enumerate(pair):
                    pltpu.make_async_copy(strip, raw.at[pl.ds(k * count, count)], sem).start()

            @pl.when(from_mine)
            def _():
                start((mine0, mine1))

            @pl.when(jnp.logical_not(from_mine))
            def _():
                start((theirs0, theirs1))

            assemble_modulation(pieces, row, blocks)
            pltpu.make_async_copy(raw, raw, sem).wait()
            project_pairs(raw, 1, row, w, last, 0, width, core)

        @pl.when(jnp.logical_not(at_end))
        def _():
            last[...] = most[bulk:]

        for strip in range(2):

            @pl.when(marked[strip])
            def _(strip=strip):
                rows = pl.ds(strip * count, count)
                early = pl.ds(0, bulk)
                group = scores.shape[0]
                for head in range(0, HEADS // 2, group):
                    attend_heads(
                        range(head, head + group), size, width, core, query.at[rows],
                        [most.at[early, :wide], last.at[:, :wide]], [most.at[early, wide:], last.at[:, wide:]],
                        None, scores, probs, whole.at[rows],
                    )

    ours = pl.ds(pl.multiple_of(count * core, count), count)
    others = pl.ds(pl.multiple_of(count * (1 - core), count), count)
    keep[...] = (near[ours] + whole[ours]).astype(BF16)
    send[...] = (near[others] + whole[others]).astype(BF16)


def output_kernel(own, keep, got, *rest, parts):
    pieces = rest[:parts]
    wo, out, blocks, row, mixed = rest[parts:]
    _, width = own.shape
    first, wide = half_columns(width)
    core = lax.rem(lax.axis_index("tile"), 2)
    assemble_modulation(pieces, row, blocks)
    low = jnp.where(core == 0, keep[...], got[...])
    high = jnp.where(core == 0, got[...], keep[...])
    mixed[:, :first] = low[:, :first]
    mixed[:, first:wide] = low[:, first:] + high[:, : wide - first]
    mixed[:, wide:] = high[:, wide - first :]
    branch = jnp.dot(mixed[...], wo[...], preferred_element_type=F32)
    gate = row[:, 2 * width : 3 * width]
    out[...] = (own[...].astype(F32) + gate * branch).astype(BF16)


def exchange_modulation(rows):
    count = len(rows)
    pieces = [rows[0]]
    for ahead in range(1, count):
        pairs = [(i, (i + ahead) % count) for i in range(count)]
        pieces.append(lax.ppermute(rows[ahead], "grp", pairs))
    return pieces


def call(kernel, outs, scratch, in_specs, flops, args, limit):
    return pl.pallas_call(
        kernel,
        out_shape=[jax.ShapeDtypeStruct(shape, dtype) for shape, dtype in outs],
        in_specs=in_specs,
        out_specs=[pl.BlockSpec(memory_space=pltpu.VMEM)] * len(outs),
        scratch_shapes=scratch,
        cost_estimate=pl.CostEstimate(flops=flops, bytes_accessed=flops // 200, transcendentals=0),
        compiler_params=pltpu.CompilerParams(vmem_limit_bytes=limit * 1024 * 1024),
    )(*args)


def on_device(latents, condition, w_modulate, w_project, w_output, detail):
    width = w_output.shape[0]
    own = latents[0]
    count = own.shape[0]
    tiles = lax.axis_size("tile")
    parts = lax.axis_size("grp")
    chips = tiles // 2
    depth = chips - 1
    _, wide = half_columns(width)
    rows = 2 * count + 2 * ROW_TOKENS
    tokens = count * tiles
    vmem = pl.BlockSpec(memory_space=pltpu.VMEM)
    anywhere = pl.BlockSpec(memory_space=pl.ANY)
    smem = pl.BlockSpec(memory_space=pltpu.SMEM)
    swap = [(i, i ^ 1) for i in range(tiles)]
    cross = [(2 * z + 1, 2 * z + 2) for z in range(chips - 1)]
    cross = cross + [(b, a) for a, b in cross]
    along = [(2 * z, 2 * z + 2) for z in range(chips - 1)]
    along = along + [(2 * z + 3, 2 * z + 1) for z in range(chips - 1)]
    mine = [lax.ppermute(own, "tile", cross), lax.ppermute(own, "tile", along)]
    partner = lax.ppermute(own, "tile", swap)
    part_width = w_modulate.shape[1]
    pieces = call(
        modulate_kernel, [((1, part_width), F32)] * parts, [], [vmem] * 2,
        10**10, (condition, w_modulate), 16,
    )
    pieces = exchange_modulation(pieces)
    for step in range(2, 2 * depth):
        mine.append(lax.ppermute(mine[step - 2], "tile", along))
    theirs = [lax.ppermute(strip, "tile", swap) for strip in mine]
    modulation = [pltpu.VMEM((parts, 1, part_width), F32), pltpu.VMEM((1, 3 * width), F32)]
    query, around = call(
        functools.partial(project_kernel, parts=parts),
        [((2 * count, wide), BF16), ((rows, 2 * wide), BF16)],
        modulation + [pltpu.VMEM((rows, width), BF16)],
        [vmem] * (5 + parts), 2 * 10**9,
        (own, partner, mine[0], theirs[0], *pieces, w_project), 16,
    )
    (near,) = call(
        functools.partial(attend_kernel, size=width // HEADS),
        [((2 * count, wide), F32)],
        [
            pltpu.VMEM((2, HEADS // 2, count, count + 2 * ROW_TOKENS), F32),
            pltpu.VMEM((2, HEADS // 2, count, count + 2 * ROW_TOKENS), BF16),
        ],
        [vmem] * 2, 10**9, (query, around), 16,
    )
    last = 2 * (depth - 1)
    early = min(depth - 1, depth)
    (most,) = call(
        functools.partial(early_kernel, parts=parts, depth=early),
        [((tokens, 2 * wide), BF16)],
        modulation + [pltpu.VMEM((tokens - 2 * count, width), BF16), pltpu.SemaphoreType.DMA],
        [anywhere] * (4 * early) + [vmem] * parts + [smem, vmem, vmem], 10**9,
        (*mine[:last], *theirs[:last], *pieces, detail, around, w_project), 12 + tokens * width * 2 // 2**20,
    )
    group = max(1, min(HEADS // 2, 2**20 // (count * tokens)))
    keep, send = call(
        functools.partial(late_kernel, parts=parts),
        [((count, wide), BF16)] * 2,
        modulation
        + [
            pltpu.VMEM((2 * count, width), BF16),
            pltpu.VMEM((2 * count, 2 * wide), BF16),
            pltpu.VMEM((2 * count, wide), F32),
            pltpu.VMEM((group, count, tokens), F32),
            pltpu.VMEM((group, count, tokens), BF16),
            pltpu.SemaphoreType.DMA,
        ],
        [anywhere] * 4 + [vmem] * parts + [smem] + [vmem] * 4, 10**9,
        (*mine[last:], *theirs[last:], *pieces, detail, query, most, near, w_project), 22,
    )
    got = lax.ppermute(send, "tile", swap)
    (updated,) = call(
        functools.partial(output_kernel, parts=parts),
        [((count, width), BF16)],
        modulation + [pltpu.VMEM((count, width), BF16)],
        [vmem] * (4 + parts), 10**9,
        (own, keep, got, *pieces, w_output), 16,
    )
    return updated[None]


def solution(mesh):
    in_specs = (P("grp", "tile", None), P(), P(None, "grp"), P(), P(), P("grp", None))
    out_specs = P("grp", "tile", None)

    return jax.shard_map(on_device, mesh=mesh, in_specs=in_specs, out_specs=out_specs, check_vma=False)
```

```python
import functools
import jax
import jax.numpy as jnp
from jax import lax
from jax.experimental import pallas as pl
from jax.experimental.pallas import tpu as pltpu
from jax.sharding import PartitionSpec as P

HEADS = 16
ROW_TOKENS = 64
LANES = 128
EPS = 1e-06
LOG2E = 1.4426950408889634
F32 = jnp.float32
BF16 = jnp.bfloat16


def half_columns(width):
    first = width // 2 // LANES * LANES
    return first, width - first


def assemble_modulation(pieces, row, blocks):
    here = lax.axis_index("grp")
    count = len(pieces)
    for back, piece in enumerate(pieces):
        blocks[lax.rem(here - back + count, count)] = piece[...]
    wide = pieces[0].shape[1]
    for block in range(count):
        row[:, block * wide : (block + 1) * wide] = blocks[block]


def normalize(rows, shift, scale):
    values = rows.astype(F32)
    mean = jnp.mean(values, axis=1, keepdims=True)
    centered = values - mean
    variance = jnp.mean(centered * centered, axis=1, keepdims=True)
    return (centered * lax.rsqrt(variance + EPS) * scale + shift).astype(BF16)


def normalize_rows(source, start, target, at, rows, shift, scale, block=32):
    for i in range(0, rows, block):
        target[pl.ds(at + i, block)] = normalize(source[pl.ds(start + i, block)], shift, scale)


def head_window(head, size, width, core):
    first, wide = half_columns(width)
    extra = width // 2 - first
    lo = head * size // LANES * LANES
    hi = min(-(-((head + 1) * size + extra) // LANES) * LANES, wide)
    column = lax.broadcasted_iota(jnp.int32, (1, hi - lo), 1) + (lo - head * size) - core * extra
    return lo, hi, (column >= 0) & (column < size)


def attend_heads(heads, size, width, core, query, keys, values, bias, scores, probs, target):
    windows = [head_window(head, size, width, core) for head in heads]
    bounds = [0]
    for key in keys:
        bounds.append(bounds[-1] + key.shape[0])
    spans = [slice(a, b) for a, b in zip(bounds, bounds[1:])]
    for head, (lo, hi, mask) in zip(heads, windows):
        part = query[:, lo:hi]
        masked = jnp.where(mask, part, jnp.zeros_like(part))
        for span, key in zip(spans, keys):
            scores[head - heads[0], :, span] = lax.dot_general(
                masked, key[:, lo:hi], (((1,), (1,)), ((), ())), preferred_element_type=F32
            )
    inverse = []
    for head in heads:
        score = scores[head - heads[0]]
        if bias is not None:
            score = score + bias
        top = jnp.max(score, axis=1, keepdims=True)
        prob = jnp.exp2((score - top) * (LOG2E / size**0.5))
        inverse.append(1.0 / jnp.sum(prob, axis=1, keepdims=True))
        probs[head - heads[0]] = prob.astype(BF16)
    for at, (head, (lo, hi, mask)) in enumerate(zip(heads, windows)):
        result = sum(
            jnp.dot(probs[at, :, span], value[:, lo:hi], preferred_element_type=F32)
            for span, value in zip(spans, values)
        )
        target[:, lo:hi] += jnp.where(mask, result * inverse[at], 0.0)


def first_kernel(out):
    out[...] = jnp.zeros_like(out)


def modulate_kernel(condition, w, _, *outs):
    columns = lax.dot_general(
        condition[...], w[...], (((1,), (1,)), ((), ())), preferred_element_type=F32
    )
    here = lax.axis_index("grp")
    count = len(outs)
    which = lax.broadcasted_iota(jnp.int32, (columns.shape[0], 1), 0)
    for ahead, out in enumerate(outs):
        out[...] = jnp.sum(
            jnp.where(which == lax.rem(here + ahead, count), columns, 0.0), axis=0, keepdims=True
        )


def project_kernel(own, partner, mine, theirs, *rest, parts):
    pieces = rest[:parts]
    w, query, kv, row, blocks, normed = rest[parts:]
    count, width = own.shape
    first, wide = half_columns(width)
    core = lax.rem(lax.axis_index("tile"), 2)
    assemble_modulation(pieces, row, blocks)
    shift = row[:, :width]
    scale = 1.0 + row[:, width : 2 * width]
    edge = ROW_TOKENS
    end = edge + 2 * count
    other = 1 - core
    normalize_rows(own, 0, normed, pl.multiple_of(edge + count * core, edge), count, shift, scale)
    normalize_rows(partner, 0, normed, pl.multiple_of(edge + count * other, edge), count, shift, scale)
    inner = count - edge
    normalize_rows(
        mine, pl.multiple_of(inner * other, edge), normed, pl.multiple_of(end * core, edge), edge, shift, scale
    )
    normalize_rows(
        theirs, pl.multiple_of(inner * core, edge), normed, pl.multiple_of(end * other, edge), edge, shift, scale
    )
    at = [pl.multiple_of(section * width + first * core, LANES) for section in range(3)]
    query[...] = jnp.dot(normed[edge:end], w[:, pl.ds(at[0], wide)], preferred_element_type=F32).astype(BF16)
    for section in (1, 2):
        part = slice((section - 1) * wide, section * wide)
        kv[:, part] = jnp.dot(normed[...], w[:, pl.ds(at[section], wide)], preferred_element_type=F32).astype(BF16)


def attend_kernel(query, kv, near, scores, probs, *, size):
    edge = ROW_TOKENS
    count = query.shape[0] // 2
    wide = query.shape[1]
    core, chip, chips = place_of_chip()
    column = lax.broadcasted_iota(jnp.int32, (1, count + 2 * edge), 1)
    near[...] = jnp.zeros_like(near)
    for strip in range(2):
        rows = pl.ds(strip * count, count)
        keys = pl.ds(strip * count, count + 2 * edge)
        if strip == 0:
            hidden = (chip == 0) & (column < edge)
        else:
            hidden = (chip == chips - 1) & (column >= count + edge)
        bias = jnp.where(hidden, -1e30, 0.0)
        attend_heads(
            range(HEADS // 2), size, size * HEADS, core, query.at[rows],
            [kv.at[keys, :wide]], [kv.at[keys, wide:]], bias, scores.at[strip], probs.at[strip], near.at[rows],
        )


def place_of_chip():
    place = lax.axis_index("tile")
    return lax.rem(place, 2), place // 2, lax.axis_size("tile") // 2


def chip_marks(marks, chip):
    return [marks[0, 2 * chip] > 0, marks[0, 2 * chip + 1] > 0]


def pair_kernel(ours0, ours1, theirs0, theirs1, row, marks, before, w, kv, normed, *, distance, first_call):
    _, chip, _ = place_of_chip()
    marked = chip_marks(marks, chip)
    count = ours0.shape[0]

    @pl.when(marked[0] | marked[1])
    def _():
        if first_call:
            kv[: 2 * count] = before[ROW_TOKENS : ROW_TOKENS + 2 * count]
        add_pairs((ours0, ours1), (theirs0, theirs1), row, w, kv, normed, distance)


def add_pairs(ours, theirs, row, w, kv, normed, distance):
    count, width = ours[0].shape
    core, chip, chips = place_of_chip()
    first, wide = half_columns(width)
    shift = row[:, :width]
    scale = 1.0 + row[:, width : 2 * width]
    lefts = chip
    rights = chips - 1 - chip
    nearer = jnp.minimum(lefts, distance - 1) + jnp.minimum(rights, distance - 1)
    for mine, pair in ((True, ours), (False, theirs)):
        is_left = (core == 0) if mine else (core == 1)
        have = jnp.where(is_left, lefts, rights) >= distance
        slot = nearer + jnp.where(is_left | (lefts < distance), 0, 1)

        @pl.when(have)
        def _(pair=pair, slot=slot):
            at = pl.multiple_of(2 * count * (slot + 1), 2 * count)
            for k, strip in enumerate(pair):
                normalize_rows(strip, 0, normed, k * count, count, shift, scale)
            for section in range(2):
                columns = pl.ds(pl.multiple_of((section + 1) * width + first * core, LANES), wide)
                kv[pl.ds(at, 2 * count), section * wide : (section + 1) * wide] = jnp.dot(
                    normed[...], w[:, columns], preferred_element_type=F32
                ).astype(BF16)


def late_kernel(
    ours0, ours1, theirs0, theirs1, row, marks, query, before, near, w,
    kv, keep, send, normed, whole, scores, probs, *, distance,
):
    count, width = ours0.shape
    _, wide = half_columns(width)
    core, chip, _ = place_of_chip()
    marked = chip_marks(marks, chip)
    whole[...] = jnp.zeros_like(whole)

    @pl.when(marked[0] | marked[1])
    def _():
        add_pairs((ours0, ours1), (theirs0, theirs1), row, w, kv, normed, distance)

    for strip in range(2):

        @pl.when(marked[strip])
        def _(strip=strip):
            rows = pl.ds(strip * count, count)
            group = scores.shape[0]
            for head in range(0, HEADS // 2, group):
                attend_heads(
                    range(head, head + group), width // HEADS, width, core, query.at[rows],
                    [kv.at[:, :wide]], [kv.at[:, wide:]], None, scores, probs, whole.at[rows],
                )

    ours = pl.ds(pl.multiple_of(count * core, count), count)
    others = pl.ds(pl.multiple_of(count * (1 - core), count), count)
    keep[...] = (near[ours] + whole[ours]).astype(BF16)
    send[...] = (near[others] + whole[others]).astype(BF16)


def output_kernel(own, keep, got, row, wo, out, mixed):
    _, width = own.shape
    first, wide = half_columns(width)
    core = lax.rem(lax.axis_index("tile"), 2)
    low = jnp.where(core == 0, keep[...], got[...])
    high = jnp.where(core == 0, got[...], keep[...])
    mixed[:, :first] = low[:, :first]
    mixed[:, first:wide] = low[:, first:] + high[:, : wide - first]
    mixed[:, wide:] = high[:, wide - first :]
    branch = jnp.dot(mixed[...], wo[...], preferred_element_type=F32)
    gate = row[:, 2 * width : 3 * width]
    out[...] = (own[...].astype(F32) + gate * branch).astype(BF16)


def exchange_modulation(rows):
    count = len(rows)
    pieces = [rows[0]]
    for ahead in range(1, count):
        pairs = [(i, (i + ahead) % count) for i in range(count)]
        pieces.append(lax.ppermute(rows[ahead], "grp", pairs))
    return pieces


def call(kernel, outs, scratch, in_specs, flops, args, limit, aliases={}):
    return pl.pallas_call(
        kernel,
        out_shape=[jax.ShapeDtypeStruct(shape, dtype) for shape, dtype in outs],
        in_specs=in_specs,
        out_specs=[pl.BlockSpec(memory_space=pltpu.VMEM)] * len(outs),
        scratch_shapes=scratch,
        input_output_aliases=aliases,
        cost_estimate=pl.CostEstimate(flops=flops, bytes_accessed=flops // 200, transcendentals=0),
        compiler_params=pltpu.CompilerParams(vmem_limit_bytes=limit * 1024 * 1024),
    )(*args)


def on_device(latents, condition, w_modulate, w_project, w_output, detail):
    width = w_output.shape[0]
    own = latents[0]
    count = own.shape[0]
    tiles = lax.axis_size("tile")
    parts = lax.axis_size("grp")
    chips = tiles // 2
    depth = chips - 1
    _, wide = half_columns(width)
    rows = 2 * count + 2 * ROW_TOKENS
    tokens = count * tiles
    vmem = pl.BlockSpec(memory_space=pltpu.VMEM)
    anywhere = pl.BlockSpec(memory_space=pl.ANY)
    smem = pl.BlockSpec(memory_space=pltpu.SMEM)
    swap = [(i, i ^ 1) for i in range(tiles)]

    def along(distance):
        right = [(2 * z - 2, 2 * z) for z in range(distance, chips)]
        return right + [(2 * z + 3, 2 * z + 1) for z in range(chips - distance)]

    cross = [(2 * z + 1, 2 * z + 2) for z in range(chips - 1)]
    cross = cross + [(b, a) for a, b in cross]
    mine = [lax.ppermute(own, "tile", cross), lax.ppermute(own, "tile", along(1))]
    partner = lax.ppermute(own, "tile", swap)
    part_width = w_modulate.shape[1]
    (token,) = call(first_kernel, [((8, LANES), F32)], [], [], 10**10, (), 16)
    pieces = call(
        modulate_kernel, [((1, part_width), F32)] * parts, [], [vmem] * 3,
        10**10, (condition, w_modulate.T, token), 16,
    )
    pieces = exchange_modulation(pieces)
    for step in range(2, 2 * depth):
        mine.append(lax.ppermute(mine[step - 2], "tile", along(step // 2 + 1)))
    theirs = [lax.ppermute(strip, "tile", swap) for strip in mine]
    query, around, row = call(
        functools.partial(project_kernel, parts=parts),
        [((2 * count, wide), BF16), ((rows, 2 * wide), BF16), ((1, 3 * width), F32)],
        [pltpu.VMEM((parts, 1, part_width), F32), pltpu.VMEM((rows, width), BF16)],
        [vmem] * (5 + parts), 2 * 10**9,
        (own, partner, mine[0], theirs[0], *pieces, w_project), 16,
    )
    (near,) = call(
        functools.partial(attend_kernel, size=width // HEADS),
        [((2 * count, wide), F32)],
        [
            pltpu.VMEM((2, HEADS // 2, count, count + 2 * ROW_TOKENS), F32),
            pltpu.VMEM((2, HEADS // 2, count, count + 2 * ROW_TOKENS), BF16),
        ],
        [vmem] * 2, 10**9, (query, around), 16,
    )
    kv = around
    kv_out = ((tokens, 2 * wide), BF16)
    pair_scratch = [pltpu.VMEM((2 * count, width), BF16)]

    def strips_at(distance):
        at = slice(2 * distance - 2, 2 * distance)
        return (*mine[at], *theirs[at])

    for distance in range(1, depth):
        (kv,) = call(
            functools.partial(pair_kernel, distance=distance, first_call=distance == 1),
            [kv_out], pair_scratch, [vmem] * 5 + [smem] + [vmem] * 2, 10**9,
            (*strips_at(distance), row, detail, kv, w_project), 12, {} if distance == 1 else {6: 0},
        )
    group = max(1, min(HEADS // 2, 2**20 // (count * tokens)))
    _, keep, send = call(
        functools.partial(late_kernel, distance=depth),
        [kv_out] + [((count, wide), BF16)] * 2,
        pair_scratch
        + [
            pltpu.VMEM((2 * count, wide), F32),
            pltpu.VMEM((group, count, tokens), F32),
            pltpu.VMEM((group, count, tokens), BF16),
        ],
        [vmem] * 5 + [smem] + [vmem] * 4, 10**9,
        (*strips_at(depth), row, detail, query, kv, near, w_project), 22, {7: 0},
    )
    got = lax.ppermute(send, "tile", swap)
    (updated,) = call(
        output_kernel, [((count, width), BF16)],
        [pltpu.VMEM((count, width), BF16)], [vmem] * 5, 10**9, (own, keep, got, row, w_output), 16,
    )
    return updated[None]


def solution(mesh):
    in_specs = (P("grp", "tile", None), P(), P(None, "grp"), P(), P(), P("grp", None))
    out_specs = P("grp", "tile", None)

    return jax.shard_map(on_device, mesh=mesh, in_specs=in_specs, out_specs=out_specs, check_vma=False)
```

```python
import functools
import jax
import jax.numpy as jnp
from jax import lax
from jax.experimental import pallas as pl
from jax.experimental.pallas import tpu as pltpu
from jax.sharding import PartitionSpec as P

HEADS = 16
ROW_TOKENS = 64
LANES = 128
EPS = 1e-06
LOG2E = 1.4426950408889634
F32 = jnp.float32
BF16 = jnp.bfloat16


def half_columns(width):
    first = width // 2 // LANES * LANES
    return first, width - first


def assemble_modulation(pieces, row, blocks):
    here = lax.axis_index("grp")
    count = len(pieces)
    for back, piece in enumerate(pieces):
        blocks[lax.rem(here - back + count, count)] = piece[...]
    wide = pieces[0].shape[1]
    for block in range(count):
        row[:, block * wide : (block + 1) * wide] = blocks[block]


def normalize(rows, shift, scale):
    values = rows.astype(F32)
    mean = jnp.mean(values, axis=1, keepdims=True)
    centered = values - mean
    variance = jnp.mean(centered * centered, axis=1, keepdims=True)
    return (centered * lax.rsqrt(variance + EPS) * scale + shift).astype(BF16)


def normalize_rows(source, start, target, at, rows, shift, scale, block=32):
    for i in range(0, rows, block):
        target[pl.ds(at + i, block)] = normalize(source[pl.ds(start + i, block)], shift, scale)


def head_window(head, size, width, core):
    first, wide = half_columns(width)
    extra = width // 2 - first
    lo = head * size // LANES * LANES
    hi = min(-(-((head + 1) * size + extra) // LANES) * LANES, wide)
    column = lax.broadcasted_iota(jnp.int32, (1, hi - lo), 1) + (lo - head * size) - core * extra
    return lo, hi, (column >= 0) & (column < size)


def attend_heads(heads, size, width, core, query, keys, values, bias, scores, probs, target):
    windows = [head_window(head, size, width, core) for head in heads]
    bounds = [0]
    for key in keys:
        bounds.append(bounds[-1] + key.shape[0])
    spans = [slice(a, b) for a, b in zip(bounds, bounds[1:])]
    for head, (lo, hi, mask) in zip(heads, windows):
        part = query[:, lo:hi]
        masked = jnp.where(mask, part, jnp.zeros_like(part))
        for span, key in zip(spans, keys):
            scores[head - heads[0], :, span] = lax.dot_general(
                masked, key[:, lo:hi], (((1,), (1,)), ((), ())), preferred_element_type=F32
            )
    inverse = []
    for head in heads:
        score = scores[head - heads[0]]
        if bias is not None:
            score = score + bias
        top = jnp.max(score, axis=1, keepdims=True)
        prob = jnp.exp2((score - top) * (LOG2E / size**0.5))
        inverse.append(1.0 / jnp.sum(prob, axis=1, keepdims=True))
        probs[head - heads[0]] = prob.astype(BF16)
    for at, (head, (lo, hi, mask)) in enumerate(zip(heads, windows)):
        result = sum(
            jnp.dot(probs[at, :, span], value[:, lo:hi], preferred_element_type=F32)
            for span, value in zip(spans, values)
        )
        target[:, lo:hi] += jnp.where(mask, result * inverse[at], 0.0)


def first_kernel(out):
    out[...] = jnp.zeros_like(out)


def modulate_kernel(condition, w, _, *outs):
    columns = lax.dot_general(
        condition[...], w[...], (((1,), (1,)), ((), ())), preferred_element_type=F32
    )
    here = lax.axis_index("grp")
    count = len(outs)
    which = lax.broadcasted_iota(jnp.int32, (columns.shape[0], 1), 0)
    for ahead, out in enumerate(outs):
        out[...] = jnp.sum(
            jnp.where(which == lax.rem(here + ahead, count), columns, 0.0), axis=0, keepdims=True
        )


def project_kernel(own, partner, mine, theirs, *rest, parts):
    pieces = rest[:parts]
    w, query, kv, row, blocks, normed = rest[parts:]
    count, width = own.shape
    first, wide = half_columns(width)
    core = lax.rem(lax.axis_index("tile"), 2)
    assemble_modulation(pieces, row, blocks)
    shift = row[:, :width]
    scale = 1.0 + row[:, width : 2 * width]
    edge = ROW_TOKENS
    end = edge + 2 * count
    other = 1 - core
    normalize_rows(own, 0, normed, pl.multiple_of(edge + count * core, edge), count, shift, scale)
    normalize_rows(partner, 0, normed, pl.multiple_of(edge + count * other, edge), count, shift, scale)
    inner = count - edge
    normalize_rows(
        mine, pl.multiple_of(inner * other, edge), normed, pl.multiple_of(end * core, edge), edge, shift, scale
    )
    normalize_rows(
        theirs, pl.multiple_of(inner * core, edge), normed, pl.multiple_of(end * other, edge), edge, shift, scale
    )
    at = [pl.multiple_of(section * width + first * core, LANES) for section in range(3)]
    query[...] = jnp.dot(normed[edge:end], w[:, pl.ds(at[0], wide)], preferred_element_type=F32).astype(BF16)
    for section in (1, 2):
        part = slice((section - 1) * wide, section * wide)
        kv[:, part] = jnp.dot(normed[...], w[:, pl.ds(at[section], wide)], preferred_element_type=F32).astype(BF16)


def attend_kernel(query, kv, near, scores, probs, *, size):
    edge = ROW_TOKENS
    count = query.shape[0] // 2
    wide = query.shape[1]
    core, chip, chips = place_of_chip()
    column = lax.broadcasted_iota(jnp.int32, (1, count + 2 * edge), 1)
    near[...] = jnp.zeros_like(near)
    for strip in range(2):
        rows = pl.ds(strip * count, count)
        keys = pl.ds(strip * count, count + 2 * edge)
        if strip == 0:
            hidden = (chip == 0) & (column < edge)
        else:
            hidden = (chip == chips - 1) & (column >= count + edge)
        bias = jnp.where(hidden, -1e30, 0.0)
        attend_heads(
            range(HEADS // 2), size, size * HEADS, core, query.at[rows],
            [kv.at[keys, :wide]], [kv.at[keys, wide:]], bias, scores.at[strip], probs.at[strip], near.at[rows],
        )


def place_of_chip():
    place = lax.axis_index("tile")
    return lax.rem(place, 2), place // 2, lax.axis_size("tile") // 2


def chip_marks(marks, chip):
    values = marks[...]
    column = lax.broadcasted_iota(jnp.int32, values.shape, 1)
    return [jnp.max(jnp.where(column == 2 * chip + core, values, 0)) > 0 for core in range(2)]


def strip_kernel(*refs, strips, distance, offset):
    ours, theirs = refs[:strips], refs[strips : 2 * strips]
    row, marks, before, w, kv, normed = refs[2 * strips :]
    _, chip, _ = place_of_chip()
    marked = chip_marks(marks, chip)
    count = ours[0].shape[0]

    @pl.when(marked[0] | marked[1])
    def _():
        if distance == 1:
            kv[: 2 * count] = before[ROW_TOKENS : ROW_TOKENS + 2 * count]
        add_pairs(ours, theirs, row, w, kv, normed, distance, offset * count)


def add_pairs(ours, theirs, row, w, kv, normed, distance, offset):
    count, width = ours[0].shape
    core, chip, chips = place_of_chip()
    first, wide = half_columns(width)
    shift = row[:, :width]
    scale = 1.0 + row[:, width : 2 * width]
    lefts = chip
    rights = chips - 1 - chip
    nearer = jnp.minimum(lefts, distance - 1) + jnp.minimum(rights, distance - 1)
    for mine, pair in ((True, ours), (False, theirs)):
        is_left = (core == 0) if mine else (core == 1)
        have = jnp.where(is_left, lefts, rights) >= distance
        slot = nearer + jnp.where(is_left | (lefts < distance), 0, 1)

        @pl.when(have)
        def _(pair=pair, slot=slot):
            at = pl.multiple_of(2 * count * (slot + 1) + offset, count)
            rows = len(pair) * count
            for k, strip in enumerate(pair):
                normalize_rows(strip, 0, normed, k * count, count, shift, scale)
            for section in range(2):
                columns = pl.ds(pl.multiple_of((section + 1) * width + first * core, LANES), wide)
                kv[pl.ds(at, rows), section * wide : (section + 1) * wide] = jnp.dot(
                    normed[:rows], w[:, columns], preferred_element_type=F32
                ).astype(BF16)


def late_kernel(
    ours, theirs, row, marks, query, before, near, w,
    kv, keep, send, normed, whole, scores, probs, *, distance,
):
    count, width = ours.shape
    _, wide = half_columns(width)
    core, chip, _ = place_of_chip()
    marked = chip_marks(marks, chip)
    whole[...] = jnp.zeros_like(whole)

    @pl.when(marked[0] | marked[1])
    def _():
        add_pairs((ours,), (theirs,), row, w, kv, normed, distance, count)

    for strip in range(2):

        @pl.when(marked[strip])
        def _(strip=strip):
            rows = pl.ds(strip * count, count)
            group = scores.shape[0]
            for head in range(0, HEADS // 2, group):
                attend_heads(
                    range(head, head + group), width // HEADS, width, core, query.at[rows],
                    [kv.at[:, :wide]], [kv.at[:, wide:]], None, scores, probs, whole.at[rows],
                )

    ours = pl.ds(pl.multiple_of(count * core, count), count)
    others = pl.ds(pl.multiple_of(count * (1 - core), count), count)
    keep[...] = (near[ours] + whole[ours]).astype(BF16)
    send[...] = (near[others] + whole[others]).astype(BF16)


def output_kernel(own, keep, got, row, wo, out, mixed):
    _, width = own.shape
    first, wide = half_columns(width)
    core = lax.rem(lax.axis_index("tile"), 2)
    low = jnp.where(core == 0, keep[...], got[...])
    high = jnp.where(core == 0, got[...], keep[...])
    mixed[:, :first] = low[:, :first]
    mixed[:, first:wide] = low[:, first:] + high[:, : wide - first]
    mixed[:, wide:] = high[:, wide - first :]
    branch = jnp.dot(mixed[...], wo[...], preferred_element_type=F32)
    gate = row[:, 2 * width : 3 * width]
    out[...] = (own[...].astype(F32) + gate * branch).astype(BF16)


def exchange_modulation(rows):
    count = len(rows)
    pieces = [rows[0]]
    for ahead in range(1, count):
        pairs = [(i, (i + ahead) % count) for i in range(count)]
        pieces.append(lax.ppermute(rows[ahead], "grp", pairs))
    return pieces


def call(kernel, outs, scratch, in_specs, flops, args, limit, aliases={}):
    return pl.pallas_call(
        kernel,
        out_shape=[jax.ShapeDtypeStruct(shape, dtype) for shape, dtype in outs],
        in_specs=in_specs,
        out_specs=[pl.BlockSpec(memory_space=pltpu.VMEM)] * len(outs),
        scratch_shapes=scratch,
        input_output_aliases=aliases,
        cost_estimate=pl.CostEstimate(flops=flops, bytes_accessed=flops // 200, transcendentals=0),
        compiler_params=pltpu.CompilerParams(vmem_limit_bytes=limit * 1024 * 1024),
    )(*args)


def on_device(latents, condition, w_modulate, w_project, w_output, detail):
    width = w_output.shape[0]
    own = latents[0]
    count = own.shape[0]
    tiles = lax.axis_size("tile")
    parts = lax.axis_size("grp")
    chips = tiles // 2
    depth = chips - 1
    _, wide = half_columns(width)
    rows = 2 * count + 2 * ROW_TOKENS
    tokens = count * tiles
    vmem = pl.BlockSpec(memory_space=pltpu.VMEM)
    swap = [(i, i ^ 1) for i in range(tiles)]

    def along(distance):
        right = [(2 * z - 2, 2 * z) for z in range(distance, chips)]
        return right + [(2 * z + 3, 2 * z + 1) for z in range(chips - distance)]

    cross = [(2 * z + 1, 2 * z + 2) for z in range(chips - 1)]
    cross = cross + [(b, a) for a, b in cross]
    mine = [lax.ppermute(own, "tile", cross), lax.ppermute(own, "tile", along(1))]
    partner = lax.ppermute(own, "tile", swap)
    part_width = w_modulate.shape[1]
    (token,) = call(first_kernel, [((8, LANES), F32)], [], [], 10**10, (), 16)
    pieces = call(
        modulate_kernel, [((1, part_width), F32)] * parts, [], [vmem] * 3,
        10**10, (condition, w_modulate.T, token), 16,
    )
    pieces = exchange_modulation(pieces)
    for step in range(2, 2 * depth):
        mine.append(lax.ppermute(mine[step - 2], "tile", along(step // 2 + 1)))
    theirs = [lax.ppermute(strip, "tile", swap) for strip in mine]
    query, around, row = call(
        functools.partial(project_kernel, parts=parts),
        [((2 * count, wide), BF16), ((rows, 2 * wide), BF16), ((1, 3 * width), F32)],
        [pltpu.VMEM((parts, 1, part_width), F32), pltpu.VMEM((rows, width), BF16)],
        [vmem] * (5 + parts), 2 * 10**9,
        (own, partner, mine[0], theirs[0], *pieces, w_project), 16,
    )
    (near,) = call(
        functools.partial(attend_kernel, size=width // HEADS),
        [((2 * count, wide), F32)],
        [
            pltpu.VMEM((2, HEADS // 2, count, count + 2 * ROW_TOKENS), F32),
            pltpu.VMEM((2, HEADS // 2, count, count + 2 * ROW_TOKENS), BF16),
        ],
        [vmem] * 2, 10**9, (query, around), 16,
    )
    kv = around
    kv_out = ((tokens, 2 * wide), BF16)
    pair_scratch = [pltpu.VMEM((2 * count, width), BF16)]

    groups = [(0, 2)] + [(at, 1) for at in range(2, len(mine) - 1)]
    for at, strips in groups:
        some = slice(at, at + strips)
        (kv,) = call(
            functools.partial(strip_kernel, strips=strips, distance=at // 2 + 1, offset=at % 2),
            [kv_out], pair_scratch, [vmem] * (2 * strips + 4), 10**9,
            (*mine[some], *theirs[some], row, detail, kv, w_project), 12,
            {} if at == 0 else {2 * strips + 2: 0},
        )
    group = max(1, min(HEADS // 2, 2**20 // (count * tokens)))
    _, keep, send = call(
        functools.partial(late_kernel, distance=depth),
        [kv_out] + [((count, wide), BF16)] * 2,
        pair_scratch
        + [
            pltpu.VMEM((2 * count, wide), F32),
            pltpu.VMEM((group, count, tokens), F32),
            pltpu.VMEM((group, count, tokens), BF16),
        ],
        [vmem] * 8, 10**9,
        (mine[-1], theirs[-1], row, detail, query, kv, near, w_project), 22, {5: 0},
    )
    got = lax.ppermute(send, "tile", swap)
    (updated,) = call(
        output_kernel, [((count, width), BF16)],
        [pltpu.VMEM((count, width), BF16)], [vmem] * 5, 10**9, (own, keep, got, row, w_output), 16,
    )
    return updated[None]


def solution(mesh):
    in_specs = (P("grp", "tile", None), P(), P(None, "grp"), P(), P(), P("grp", None))
    out_specs = P("grp", "tile", None)

    return jax.shard_map(on_device, mesh=mesh, in_specs=in_specs, out_specs=out_specs, check_vma=False)
```

```python
import functools
import jax
import jax.numpy as jnp
from jax import lax
from jax.experimental import pallas as pl
from jax.experimental.pallas import tpu as pltpu
from jax.sharding import PartitionSpec as P

HEADS = 16
ROW_TOKENS = 64
LANES = 128
EPS = 1e-06
LOG2E = 1.4426950408889634
F32 = jnp.float32
BF16 = jnp.bfloat16


def half_columns(width):
    first = width // 2 // LANES * LANES
    return first, width - first


def assemble_modulation(pieces, row, blocks):
    here = lax.axis_index("grp")
    count = len(pieces)
    for bits, piece in enumerate(pieces):
        blocks[lax.bitwise_xor(here, bits)] = piece[...]
    wide = pieces[0].shape[1]
    for block in range(count):
        row[:, block * wide : (block + 1) * wide] = blocks[block]


def normalize(rows, shift, scale):
    values = rows.astype(F32)
    mean = jnp.mean(values, axis=1, keepdims=True)
    centered = values - mean
    variance = jnp.mean(centered * centered, axis=1, keepdims=True)
    return (centered * lax.rsqrt(variance + EPS) * scale + shift).astype(BF16)


def normalize_rows(source, start, target, at, rows, shift, scale, block=32):
    for i in range(0, rows, block):
        target[pl.ds(at + i, block)] = normalize(source[pl.ds(start + i, block)], shift, scale)


def head_window(head, size, width, core):
    first, wide = half_columns(width)
    extra = width // 2 - first
    lo = head * size // LANES * LANES
    hi = min(-(-((head + 1) * size + extra) // LANES) * LANES, wide)
    column = lax.broadcasted_iota(jnp.int32, (1, hi - lo), 1) + (lo - head * size) - core * extra
    return lo, hi, (column >= 0) & (column < size)


def attend_heads(heads, size, width, core, query, keys, values, bias, scores, probs, target):
    windows = [head_window(head, size, width, core) for head in heads]
    bounds = [0]
    for key in keys:
        bounds.append(bounds[-1] + key.shape[0])
    spans = [slice(a, b) for a, b in zip(bounds, bounds[1:])]
    for head, (lo, hi, mask) in zip(heads, windows):
        part = query[:, lo:hi]
        masked = jnp.where(mask, part, jnp.zeros_like(part))
        for span, key in zip(spans, keys):
            scores[head - heads[0], :, span] = lax.dot_general(
                masked, key[:, lo:hi], (((1,), (1,)), ((), ())), preferred_element_type=F32
            )
    inverse = []
    for head in heads:
        score = scores[head - heads[0]]
        if bias is not None:
            score = score + bias
        top = jnp.max(score, axis=1, keepdims=True)
        prob = jnp.exp2((score - top) * (LOG2E / size**0.5))
        inverse.append(1.0 / jnp.sum(prob, axis=1, keepdims=True))
        probs[head - heads[0]] = prob.astype(BF16)
    for at, (head, (lo, hi, mask)) in enumerate(zip(heads, windows)):
        result = sum(
            jnp.dot(probs[at, :, span], value[:, lo:hi], preferred_element_type=F32)
            for span, value in zip(spans, values)
        )
        target[:, lo:hi] += jnp.where(mask, result * inverse[at], 0.0)


def first_kernel(out):
    out[...] = jnp.zeros_like(out)


def modulate_kernel(condition, w, _, *outs):
    columns = lax.dot_general(
        condition[...], w[...], (((1,), (1,)), ((), ())), preferred_element_type=F32
    )
    here = lax.axis_index("grp")
    which = lax.broadcasted_iota(jnp.int32, (columns.shape[0], 1), 0)
    for bits, out in enumerate(outs):
        out[...] = jnp.sum(
            jnp.where(which == lax.bitwise_xor(here, bits), columns, 0.0), axis=0, keepdims=True
        )


def project_kernel(own, partner, *rest, parts):
    pieces = rest[:parts]
    w, query, kv, row, blocks, normed = rest[parts:]
    count, width = own.shape
    first, wide = half_columns(width)
    core = lax.rem(lax.axis_index("tile"), 2)
    assemble_modulation(pieces, row, blocks)
    shift = row[:, :width]
    scale = 1.0 + row[:, width : 2 * width]
    normalize_rows(own, 0, normed, pl.multiple_of(count * core, count), count, shift, scale)
    normalize_rows(partner, 0, normed, pl.multiple_of(count * (1 - core), count), count, shift, scale)
    for section, (target, to) in enumerate(((query, 0), (kv, 0), (kv, wide))):
        at = pl.multiple_of(section * width + first * core, LANES)
        target[:, to : to + wide] = jnp.dot(
            normed[...], w[:, pl.ds(at, wide)], preferred_element_type=F32
        ).astype(BF16)


def attend_kernel(mine, theirs, row, query, pairs, w, near, normed, kv, scores, probs):
    edge = ROW_TOKENS
    count, width = mine.shape
    first, wide = half_columns(width)
    core, chip, chips = place_of_chip()
    other = 1 - core
    inner = count - edge
    end = edge + 2 * count
    shift = row[:, :width]
    scale = 1.0 + row[:, width : 2 * width]
    normalize_rows(
        mine, pl.multiple_of(inner * other, edge), normed, pl.multiple_of(edge * core, edge), edge, shift, scale
    )
    normalize_rows(
        theirs, pl.multiple_of(inner * core, edge), normed, pl.multiple_of(edge * other, edge), edge, shift, scale
    )
    kv[edge:end] = pairs[...]
    for section in range(2):
        at = pl.multiple_of((section + 1) * width + first * core, LANES)
        margins = jnp.dot(normed[...], w[:, pl.ds(at, wide)], preferred_element_type=F32).astype(BF16)
        part = slice(section * wide, (section + 1) * wide)
        kv[:edge, part] = margins[:edge]
        kv[end:, part] = margins[edge:]
    column = lax.broadcasted_iota(jnp.int32, (1, count + 2 * edge), 1)
    near[...] = jnp.zeros_like(near)
    for strip in range(2):
        rows = pl.ds(strip * count, count)
        keys = pl.ds(strip * count, count + 2 * edge)
        if strip == 0:
            hidden = (chip == 0) & (column < edge)
        else:
            hidden = (chip == chips - 1) & (column >= count + edge)
        bias = jnp.where(hidden, -1e30, 0.0)
        attend_heads(
            range(HEADS // 2), width // HEADS, width, core, query.at[rows],
            [kv.at[keys, :wide]], [kv.at[keys, wide:]], bias, scores.at[strip], probs.at[strip], near.at[rows],
        )


def place_of_chip():
    place = lax.axis_index("tile")
    return lax.rem(place, 2), place // 2, lax.axis_size("tile") // 2


def chip_marks(marks, chip):
    values = marks[...]
    column = lax.broadcasted_iota(jnp.int32, values.shape, 1)
    return [jnp.max(jnp.where(column == 2 * chip + core, values, 0)) > 0 for core in range(2)]


def strip_kernel(ours, theirs, row, marks, before, w, kv, normed, *, distance, offset):
    _, chip, _ = place_of_chip()
    marked = chip_marks(marks, chip)
    count = ours.shape[0]

    @pl.when(marked[0] | marked[1])
    def _():
        if distance == 1 and offset == 0:
            kv[: 2 * count] = before[...]
        add_strips(ours, theirs, row, w, kv, normed, distance, offset * count)


def add_strips(ours, theirs, row, w, kv, normed, distance, offset):
    count, width = ours.shape
    core, chip, chips = place_of_chip()
    first, wide = half_columns(width)
    shift = row[:, :width]
    scale = 1.0 + row[:, width : 2 * width]
    lefts = chip
    rights = chips - 1 - chip
    nearer = jnp.minimum(lefts, distance - 1) + jnp.minimum(rights, distance - 1)
    for mine, strip in ((True, ours), (False, theirs)):
        is_left = (core == 0) if mine else (core == 1)
        have = jnp.where(is_left, lefts, rights) >= distance
        slot = nearer + jnp.where(is_left | (lefts < distance), 0, 1)

        @pl.when(have)
        def _(strip=strip, slot=slot):
            at = pl.multiple_of(2 * count * (slot + 1) + offset, count)
            normalize_rows(strip, 0, normed, 0, count, shift, scale)
            for section in range(2):
                columns = pl.ds(pl.multiple_of((section + 1) * width + first * core, LANES), wide)
                kv[pl.ds(at, count), section * wide : (section + 1) * wide] = jnp.dot(
                    normed[...], w[:, columns], preferred_element_type=F32
                ).astype(BF16)


def late_kernel(
    ours, theirs, row, marks, query, before, near, w,
    kv, keep, send, normed, whole, scores, probs, *, distance,
):
    count, width = ours.shape
    _, wide = half_columns(width)
    core, chip, _ = place_of_chip()
    marked = chip_marks(marks, chip)
    whole[...] = jnp.zeros_like(whole)

    @pl.when(marked[0] | marked[1])
    def _():
        add_strips(ours, theirs, row, w, kv, normed, distance, count)

    for strip in range(2):

        @pl.when(marked[strip])
        def _(strip=strip):
            rows = pl.ds(strip * count, count)
            group = scores.shape[0]
            for head in range(0, HEADS // 2, group):
                attend_heads(
                    range(head, head + group), width // HEADS, width, core, query.at[rows],
                    [kv.at[:, :wide]], [kv.at[:, wide:]], None, scores, probs, whole.at[rows],
                )

    ours = pl.ds(pl.multiple_of(count * core, count), count)
    others = pl.ds(pl.multiple_of(count * (1 - core), count), count)
    keep[...] = (near[ours] + whole[ours]).astype(BF16)
    send[...] = (near[others] + whole[others]).astype(BF16)


def output_kernel(own, keep, got, row, wo, out, mixed):
    _, width = own.shape
    first, wide = half_columns(width)
    core = lax.rem(lax.axis_index("tile"), 2)
    low = jnp.where(core == 0, keep[...], got[...])
    high = jnp.where(core == 0, got[...], keep[...])
    mixed[:, :first] = low[:, :first]
    mixed[:, first:wide] = low[:, first:] + high[:, : wide - first]
    mixed[:, wide:] = high[:, wide - first :]
    branch = jnp.dot(mixed[...], wo[...], preferred_element_type=F32)
    gate = row[:, 2 * width : 3 * width]
    out[...] = (own[...].astype(F32) + gate * branch).astype(BF16)


def exchange_modulation(rows):
    count = len(rows)
    pieces = [rows[0]]
    for bits in range(1, count):
        pairs = [(i, i ^ bits) for i in range(count)]
        pieces.append(lax.ppermute(rows[bits], "grp", pairs))
    return pieces


def call(kernel, outs, scratch, in_specs, flops, args, limit, aliases={}):
    return pl.pallas_call(
        kernel,
        out_shape=[jax.ShapeDtypeStruct(shape, dtype) for shape, dtype in outs],
        in_specs=in_specs,
        out_specs=[pl.BlockSpec(memory_space=pltpu.VMEM)] * len(outs),
        scratch_shapes=scratch,
        input_output_aliases=aliases,
        cost_estimate=pl.CostEstimate(flops=flops, bytes_accessed=flops // 200, transcendentals=0),
        compiler_params=pltpu.CompilerParams(vmem_limit_bytes=limit * 1024 * 1024),
    )(*args)


def on_device(latents, condition, w_modulate, w_project, w_output, detail):
    width = w_output.shape[0]
    own = latents[0]
    count = own.shape[0]
    tiles = lax.axis_size("tile")
    parts = lax.axis_size("grp")
    chips = tiles // 2
    depth = chips - 1
    _, wide = half_columns(width)
    rows = 2 * count + 2 * ROW_TOKENS
    tokens = count * tiles
    vmem = pl.BlockSpec(memory_space=pltpu.VMEM)
    swap = [(i, i ^ 1) for i in range(tiles)]

    def along(distance):
        right = [(2 * z - 2, 2 * z) for z in range(distance, chips)]
        return right + [(2 * z + 3, 2 * z + 1) for z in range(chips - distance)]

    cross = [(2 * z + 1, 2 * z + 2) for z in range(chips - 1)]
    cross = cross + [(b, a) for a, b in cross]
    mine = [lax.ppermute(own, "tile", cross), lax.ppermute(own, "tile", along(1))]
    partner = lax.ppermute(own, "tile", swap)
    part_width = w_modulate.shape[1]
    (token,) = call(first_kernel, [((8, LANES), F32)], [], [], 10**10, (), 16)
    pieces = call(
        modulate_kernel, [((1, part_width), F32)] * parts, [], [vmem] * 3,
        10**10, (condition, w_modulate.T, token), 16,
    )
    pieces = exchange_modulation(pieces)
    for step in range(2, 2 * depth):
        mine.append(lax.ppermute(mine[step - 2], "tile", along(step // 2 + 1)))
    theirs = [lax.ppermute(strip, "tile", swap) for strip in mine]
    query, kv, row = call(
        functools.partial(project_kernel, parts=parts),
        [((2 * count, wide), BF16), ((2 * count, 2 * wide), BF16), ((1, 3 * width), F32)],
        [pltpu.VMEM((parts, 1, part_width), F32), pltpu.VMEM((2 * count, width), BF16)],
        [vmem] * (3 + parts), 2 * 10**9, (own, partner, *pieces, w_project), 16,
    )
    (near,) = call(
        attend_kernel,
        [((2 * count, wide), F32)],
        [
            pltpu.VMEM((2 * ROW_TOKENS, width), BF16),
            pltpu.VMEM((rows, 2 * wide), BF16),
            pltpu.VMEM((2, HEADS // 2, count, count + 2 * ROW_TOKENS), F32),
            pltpu.VMEM((2, HEADS // 2, count, count + 2 * ROW_TOKENS), BF16),
        ],
        [vmem] * 6, 10**9, (mine[0], theirs[0], row, query, kv, w_project), 16,
    )
    kv_out = ((tokens, 2 * wide), BF16)
    pair_scratch = [pltpu.VMEM((count, width), BF16)]

    for at in range(len(mine) - 1):
        (kv,) = call(
            functools.partial(strip_kernel, distance=at // 2 + 1, offset=at % 2),
            [kv_out], pair_scratch, [vmem] * 6, 10**9,
            (mine[at], theirs[at], row, detail, kv, w_project), 12, {} if at == 0 else {4: 0},
        )
    group = max(1, min(HEADS // 2, 2**20 // (count * tokens)))
    _, keep, send = call(
        functools.partial(late_kernel, distance=depth),
        [kv_out] + [((count, wide), BF16)] * 2,
        pair_scratch
        + [
            pltpu.VMEM((2 * count, wide), F32),
            pltpu.VMEM((group, count, tokens), F32),
            pltpu.VMEM((group, count, tokens), BF16),
        ],
        [vmem] * 8, 10**9,
        (mine[-1], theirs[-1], row, detail, query, kv, near, w_project), 22, {5: 0},
    )
    got = lax.ppermute(send, "tile", swap)
    (updated,) = call(
        output_kernel, [((count, width), BF16)],
        [pltpu.VMEM((count, width), BF16)], [vmem] * 5, 10**9, (own, keep, got, row, w_output), 16,
    )
    return updated[None]


def solution(mesh):
    in_specs = (P("grp", "tile", None), P(), P(None, "grp"), P(), P(), P("grp", None))
    out_specs = P("grp", "tile", None)

    return jax.shard_map(on_device, mesh=mesh, in_specs=in_specs, out_specs=out_specs, check_vma=False)
```

```python
import functools
import jax
import jax.numpy as jnp
from jax import lax
from jax.experimental import pallas as pl
from jax.experimental.pallas import tpu as pltpu
from jax.sharding import PartitionSpec as P

HEADS = 16
ROW_TOKENS = 64
LANES = 128
EPS = 1e-06
LOG2E = 1.4426950408889634
F32 = jnp.float32
BF16 = jnp.bfloat16


def half_columns(width):
    first = width // 2 // LANES * LANES
    return first, width - first


def assemble_modulation(pieces, row, blocks):
    here = lax.axis_index("grp")
    count = len(pieces)
    for bits, piece in enumerate(pieces):
        blocks[lax.bitwise_xor(here, bits)] = piece[...]
    wide = pieces[0].shape[1]
    for block in range(count):
        row[:, block * wide : (block + 1) * wide] = blocks[block]


def normalize(rows, shift, scale):
    values = rows.astype(F32)
    mean = jnp.mean(values, axis=1, keepdims=True)
    centered = values - mean
    variance = jnp.mean(centered * centered, axis=1, keepdims=True)
    return (centered * lax.rsqrt(variance + EPS) * scale + shift).astype(BF16)


def normalize_rows(source, start, target, at, rows, shift, scale, block=32):
    for i in range(0, rows, block):
        target[pl.ds(at + i, block)] = normalize(source[pl.ds(start + i, block)], shift, scale)


def head_window(head, size, width, core):
    first, wide = half_columns(width)
    extra = width // 2 - first
    lo = head * size // LANES * LANES
    hi = min(-(-((head + 1) * size + extra) // LANES) * LANES, wide)
    column = lax.broadcasted_iota(jnp.int32, (1, hi - lo), 1) + (lo - head * size) - core * extra
    return lo, hi, (column >= 0) & (column < size)


def attend_heads(heads, size, width, core, query, keys, values, bias, scores, probs, target):
    windows = [head_window(head, size, width, core) for head in heads]
    bounds = [0]
    for key in keys:
        bounds.append(bounds[-1] + key.shape[0])
    spans = [slice(a, b) for a, b in zip(bounds, bounds[1:])]
    for head, (lo, hi, mask) in zip(heads, windows):
        part = query[:, lo:hi]
        masked = jnp.where(mask, part, jnp.zeros_like(part))
        for span, key in zip(spans, keys):
            scores[head - heads[0], :, span] = lax.dot_general(
                masked, key[:, lo:hi], (((1,), (1,)), ((), ())), preferred_element_type=F32
            )
    inverse = []
    for head in heads:
        score = scores[head - heads[0]]
        if bias is not None:
            score = score + bias
        top = jnp.max(score, axis=1, keepdims=True)
        prob = jnp.exp2((score - top) * (LOG2E / size**0.5))
        inverse.append(1.0 / jnp.sum(prob, axis=1, keepdims=True))
        probs[head - heads[0]] = prob.astype(BF16)
    for at, (head, (lo, hi, mask)) in enumerate(zip(heads, windows)):
        result = sum(
            jnp.dot(probs[at, :, span], value[:, lo:hi], preferred_element_type=F32)
            for span, value in zip(spans, values)
        )
        target[:, lo:hi] += jnp.where(mask, result * inverse[at], 0.0)


def first_kernel(out):
    out[...] = jnp.zeros_like(out)


def modulate_kernel(condition, w, _, *outs):
    columns = lax.dot_general(
        condition[...], w[...], (((1,), (1,)), ((), ())), preferred_element_type=F32
    )
    here = lax.axis_index("grp")
    which = lax.broadcasted_iota(jnp.int32, (columns.shape[0], 1), 0)
    for bits, out in enumerate(outs):
        out[...] = jnp.sum(
            jnp.where(which == lax.bitwise_xor(here, bits), columns, 0.0), axis=0, keepdims=True
        )


def project_kernel(own, partner, *rest, parts):
    pieces = rest[:parts]
    w, query, kv, row, blocks, normed = rest[parts:]
    count, width = own.shape
    first, wide = half_columns(width)
    core = lax.rem(lax.axis_index("tile"), 2)
    assemble_modulation(pieces, row, blocks)
    shift = row[:, :width]
    scale = 1.0 + row[:, width : 2 * width]
    normalize_rows(own, 0, normed, pl.multiple_of(count * core, count), count, shift, scale)
    normalize_rows(partner, 0, normed, pl.multiple_of(count * (1 - core), count), count, shift, scale)
    for section, (target, to) in enumerate(((query, 0), (kv, 0), (kv, wide))):
        at = pl.multiple_of(section * width + first * core, LANES)
        target[:, to : to + wide] = jnp.dot(
            normed[...], w[:, pl.ds(at, wide)], preferred_element_type=F32
        ).astype(BF16)


def attend_kernel(mine, theirs, row, query, pairs, w, near, normed, kv, scores, probs):
    edge = ROW_TOKENS
    count, width = mine.shape
    first, wide = half_columns(width)
    core, chip, chips = place_of_chip()
    other = 1 - core
    inner = count - edge
    end = edge + 2 * count
    shift = row[:, :width]
    scale = 1.0 + row[:, width : 2 * width]
    normalize_rows(
        mine, pl.multiple_of(inner * other, edge), normed, pl.multiple_of(edge * core, edge), edge, shift, scale
    )
    normalize_rows(
        theirs, pl.multiple_of(inner * core, edge), normed, pl.multiple_of(edge * other, edge), edge, shift, scale
    )
    kv[edge:end] = pairs[...]
    for section in range(2):
        at = pl.multiple_of((section + 1) * width + first * core, LANES)
        margins = jnp.dot(normed[...], w[:, pl.ds(at, wide)], preferred_element_type=F32).astype(BF16)
        part = slice(section * wide, (section + 1) * wide)
        kv[:edge, part] = margins[:edge]
        kv[end:, part] = margins[edge:]
    column = lax.broadcasted_iota(jnp.int32, (1, count + 2 * edge), 1)
    near[...] = jnp.zeros_like(near)
    for strip in range(2):
        rows = pl.ds(strip * count, count)
        keys = pl.ds(strip * count, count + 2 * edge)
        if strip == 0:
            hidden = (chip == 0) & (column < edge)
        else:
            hidden = (chip == chips - 1) & (column >= count + edge)
        bias = jnp.where(hidden, -1e30, 0.0)
        attend_heads(
            range(HEADS // 2), width // HEADS, width, core, query.at[rows],
            [kv.at[keys, :wide]], [kv.at[keys, wide:]], bias, scores.at[strip], probs.at[strip], near.at[rows],
        )


def place_of_chip():
    place = lax.axis_index("tile")
    return lax.rem(place, 2), place // 2, lax.axis_size("tile") // 2


def chip_marks(marks, chip):
    values = marks[...]
    column = lax.broadcasted_iota(jnp.int32, values.shape, 1)
    return [jnp.max(jnp.where(column == 2 * chip + core, values, 0)) > 0 for core in range(2)]


def strip_kernel(ours, theirs, row, marks, before, w, kv, normed, *, distance, offset):
    _, chip, _ = place_of_chip()
    marked = chip_marks(marks, chip)
    count = ours.shape[0]

    @pl.when(marked[0] | marked[1])
    def _():
        if distance == 1 and offset == 0:
            kv[: 2 * count] = before[...]
        add_strips(ours, theirs, row, w, kv, normed, distance, offset * count)


def add_strips(ours, theirs, row, w, kv, normed, distance, offset):
    count, width = ours.shape
    core, chip, chips = place_of_chip()
    first, wide = half_columns(width)
    shift = row[:, :width]
    scale = 1.0 + row[:, width : 2 * width]
    lefts = chip
    rights = chips - 1 - chip
    nearer = jnp.minimum(lefts, distance - 1) + jnp.minimum(rights, distance - 1)
    for mine, strip in ((True, ours), (False, theirs)):
        is_left = (core == 0) if mine else (core == 1)
        have = jnp.where(is_left, lefts, rights) >= distance
        slot = nearer + jnp.where(is_left | (lefts < distance), 0, 1)

        @pl.when(have)
        def _(strip=strip, slot=slot):
            at = pl.multiple_of(2 * count * (slot + 1) + offset, count)
            normalize_rows(strip, 0, normed, 0, count, shift, scale)
            for section in range(2):
                columns = pl.ds(pl.multiple_of((section + 1) * width + first * core, LANES), wide)
                kv[pl.ds(at, count), section * wide : (section + 1) * wide] = jnp.dot(
                    normed[...], w[:, columns], preferred_element_type=F32
                ).astype(BF16)


def late_kernel(
    ours, theirs, row, marks, query, before, near, w,
    kv, keep, send, normed, whole, scores, probs, *, distance,
):
    count, width = ours.shape
    _, wide = half_columns(width)
    core, chip, _ = place_of_chip()
    marked = chip_marks(marks, chip)
    whole[...] = jnp.zeros_like(whole)

    @pl.when(marked[0] | marked[1])
    def _():
        add_strips(ours, theirs, row, w, kv, normed, distance, count)

    def attend_rows(rows, height):
        group = scores.shape[0]
        for head in range(0, HEADS // 2, group):
            attend_heads(
                range(head, head + group), width // HEADS, width, core, query.at[rows],
                [kv.at[:, :wide]], [kv.at[:, wide:]], None,
                scores.at[:, pl.ds(0, height)], probs.at[:, pl.ds(0, height)], whole.at[rows],
            )

    if scores.shape[1] > count:

        @pl.when(marked[0] & marked[1])
        def _():
            attend_rows(pl.ds(0, 2 * count), 2 * count)

        @pl.when(marked[0] != marked[1])
        def _():
            attend_rows(pl.ds(pl.multiple_of(jnp.where(marked[0], 0, count), count), count), count)
    else:
        for strip in range(2):

            @pl.when(marked[strip])
            def _(strip=strip):
                attend_rows(pl.ds(strip * count, count), count)

    ours = pl.ds(pl.multiple_of(count * core, count), count)
    others = pl.ds(pl.multiple_of(count * (1 - core), count), count)
    keep[...] = (near[ours] + whole[ours]).astype(BF16)
    send[...] = (near[others] + whole[others]).astype(BF16)


def output_kernel(own, keep, got, row, wo, out, mixed):
    _, width = own.shape
    first, wide = half_columns(width)
    core = lax.rem(lax.axis_index("tile"), 2)
    low = jnp.where(core == 0, keep[...], got[...])
    high = jnp.where(core == 0, got[...], keep[...])
    mixed[:, :first] = low[:, :first]
    mixed[:, first:wide] = low[:, first:] + high[:, : wide - first]
    mixed[:, wide:] = high[:, wide - first :]
    branch = jnp.dot(mixed[...], wo[...], preferred_element_type=F32)
    gate = row[:, 2 * width : 3 * width]
    out[...] = (own[...].astype(F32) + gate * branch).astype(BF16)


def exchange_modulation(rows):
    count = len(rows)
    pieces = [rows[0]]
    for bits in range(1, count):
        pairs = [(i, i ^ bits) for i in range(count)]
        pieces.append(lax.ppermute(rows[bits], "grp", pairs))
    return pieces


def call(kernel, outs, scratch, in_specs, flops, args, limit, aliases={}):
    return pl.pallas_call(
        kernel,
        out_shape=[jax.ShapeDtypeStruct(shape, dtype) for shape, dtype in outs],
        in_specs=in_specs,
        out_specs=[pl.BlockSpec(memory_space=pltpu.VMEM)] * len(outs),
        scratch_shapes=scratch,
        input_output_aliases=aliases,
        cost_estimate=pl.CostEstimate(flops=flops, bytes_accessed=flops // 200, transcendentals=0),
        compiler_params=pltpu.CompilerParams(vmem_limit_bytes=limit * 1024 * 1024),
    )(*args)


def on_device(latents, condition, w_modulate, w_project, w_output, detail):
    width = w_output.shape[0]
    own = latents[0]
    count = own.shape[0]
    tiles = lax.axis_size("tile")
    parts = lax.axis_size("grp")
    chips = tiles // 2
    depth = chips - 1
    _, wide = half_columns(width)
    rows = 2 * count + 2 * ROW_TOKENS
    tokens = count * tiles
    vmem = pl.BlockSpec(memory_space=pltpu.VMEM)
    swap = [(i, i ^ 1) for i in range(tiles)]

    def along(distance):
        right = [(2 * z - 2, 2 * z) for z in range(distance, chips)]
        return right + [(2 * z + 3, 2 * z + 1) for z in range(chips - distance)]

    cross = [(2 * z + 1, 2 * z + 2) for z in range(chips - 1)]
    cross = cross + [(b, a) for a, b in cross]
    mine = [lax.ppermute(own, "tile", cross), lax.ppermute(own, "tile", along(1))]
    partner = lax.ppermute(own, "tile", swap)
    part_width = w_modulate.shape[1]
    (token,) = call(first_kernel, [((8, LANES), F32)], [], [], 10**10, (), 16)
    pieces = call(
        modulate_kernel, [((1, part_width), F32)] * parts, [], [vmem] * 3,
        10**10, (condition, w_modulate.T, token), 16,
    )
    pieces = exchange_modulation(pieces)
    for step in range(2, 2 * depth):
        mine.append(lax.ppermute(mine[step - 2], "tile", along(step // 2 + 1)))
    theirs = [lax.ppermute(strip, "tile", swap) for strip in mine]
    query, kv, row = call(
        functools.partial(project_kernel, parts=parts),
        [((2 * count, wide), BF16), ((2 * count, 2 * wide), BF16), ((1, 3 * width), F32)],
        [pltpu.VMEM((parts, 1, part_width), F32), pltpu.VMEM((2 * count, width), BF16)],
        [vmem] * (3 + parts), 2 * 10**9, (own, partner, *pieces, w_project), 16,
    )
    (near,) = call(
        attend_kernel,
        [((2 * count, wide), F32)],
        [
            pltpu.VMEM((2 * ROW_TOKENS, width), BF16),
            pltpu.VMEM((rows, 2 * wide), BF16),
            pltpu.VMEM((2, HEADS // 2, count, count + 2 * ROW_TOKENS), F32),
            pltpu.VMEM((2, HEADS // 2, count, count + 2 * ROW_TOKENS), BF16),
        ],
        [vmem] * 6, 10**9, (mine[0], theirs[0], row, query, kv, w_project), 16,
    )
    kv_out = ((tokens, 2 * wide), BF16)
    pair_scratch = [pltpu.VMEM((count, width), BF16)]

    for at in range(len(mine) - 1):
        (kv,) = call(
            functools.partial(strip_kernel, distance=at // 2 + 1, offset=at % 2),
            [kv_out], pair_scratch, [vmem] * 6, 10**9,
            (mine[at], theirs[at], row, detail, kv, w_project), 12, {} if at == 0 else {4: 0},
        )
    group = max(1, min(HEADS // 2, 2**20 // (count * tokens)))
    height = 2 * count if group == HEADS // 2 else count
    _, keep, send = call(
        functools.partial(late_kernel, distance=depth),
        [kv_out] + [((count, wide), BF16)] * 2,
        pair_scratch
        + [
            pltpu.VMEM((2 * count, wide), F32),
            pltpu.VMEM((group, height, tokens), F32),
            pltpu.VMEM((group, height, tokens), BF16),
        ],
        [vmem] * 8, 10**9,
        (mine[-1], theirs[-1], row, detail, query, kv, near, w_project), 30 if height > count else 22, {5: 0},
    )
    got = lax.ppermute(send, "tile", swap)
    (updated,) = call(
        output_kernel, [((count, width), BF16)],
        [pltpu.VMEM((count, width), BF16)], [vmem] * 5, 10**9, (own, keep, got, row, w_output), 16,
    )
    return updated[None]


def solution(mesh):
    in_specs = (P("grp", "tile", None), P(), P(None, "grp"), P(), P(), P("grp", None))
    out_specs = P("grp", "tile", None)

    return jax.shard_map(on_device, mesh=mesh, in_specs=in_specs, out_specs=out_specs, check_vma=False)
```
